32 devices in a mesh: dp: 16 (over z, x, core), mp: 2 (over y).
Axes of the slice: x: 2, y: 2, z: 4, core: 2. Of those that a mesh axis runs over, the one named last changes fastest.
Arguments:
- ranges: bfloat16 [512, 2652], P(('dp', 'mp')), may hold values from 0.0099487305 to 1
- board: int32 [512, 5], P(('dp', 'mp')), may hold values from 0 to 51, as said below
- targets: bfloat16 [512, 2652], P(('dp', 'mp')), may hold values from -6 to 6
- w_in: bfloat16 [1536, 2704], P(('mp', 'dp')), may hold values from -0.34570312 to 0.34570312
- w_out: bfloat16 [1536, 2652], P(('mp', 'dp')), may hold values from -0.3046875 to 0.3046875
Outputs:
- predicted: bfloat16 [512, 2652], P(('dp', 'mp'))
- update_in: float32 [1536, 2704], P(('mp', 'dp'))
- update_out: float32 [1536, 2652], P(('mp', 'dp'))
- loss: float32 [], replicated
The draws below stay inside these ranges and needn't reach their ends.
Inputs may be any that keep to these rules, and one draw needn't show every extreme that they name: `board`: each row holds 5 different cards.
All inputs are finite; a program needn't handle non-finite values.
Results may differ from the reference program's by a relative error of at most 0.014.
Values may be sent and summed in bfloat16 or wider, within the bound.
No kernel may reach another device: no remote copies, remote signals or barrier semaphores. Data moves between devices by JAX's collectives and lax.ppermute only.
A program may use at most 64 MiB of HBM per device.

```python
import math
import jax
import jax.numpy as jnp
from jax import lax

CARDS = 52
BOARD = 5
HIDDEN_SIZE = 1536
INW = 2704
OUTW = 2652
BATCH = 512
N_MP = 2


def draw_board(key, part):
    row_keys = jax.random.split(key, BATCH)

    def one_board(row_key):
        return jax.random.permutation(row_key, CARDS)[:BOARD]
    return jax.vmap(one_board)(row_keys).astype(jnp.int32)


def block_levels(key, shape, pieces, low, high):
    factor_of = 1.0
    for dim, blocks in pieces:
        draws = jax.random.uniform(jax.random.fold_in(jax.random.fold_in(key, 6), dim), (blocks,), jnp.float32, low / len(pieces), high / len(pieces))
        factor_of = factor_of * jnp.repeat(jnp.exp(draws), shape[dim] // blocks).reshape((-1,) + (1,) * (len(shape) - 1 - dim))
    return factor_of


def normal_values(stream_key, extent, width, most, shards=(), kind=jnp.bfloat16):
    gain = block_levels(stream_key, extent, shards, -0.22, 0.18) if shards else 1.0
    result = jax.random.normal(stream_key, extent, jnp.float32) * width * gain
    return jnp.minimum(jnp.maximum(result, -most), most).astype(kind)


def setup_inputs(seed: int = 0) -> dict:
    keys = jax.random.split(jax.random.key(seed), 6)
    return {
        "ranges": jnp.clip(jnp.exp(math.log(1.0) - 4.61031033 * jax.random.uniform(keys[0], (BATCH, OUTW), jnp.float32) ** block_levels(keys[0], (BATCH, OUTW), ((0, 32),), -0.2, 0.2)), 0.0099487305, 1.0).astype(jnp.bfloat16),
        "board": draw_board(jax.random.fold_in(keys[5], 71), 0),
        "targets": normal_values(keys[2], (BATCH, OUTW), 1.0, 6.0, ((0, 32),)),
        "w_in": normal_values(keys[3], (HIDDEN_SIZE, INW), (3.0 * INW ** -0.5), 0.34570312, ((0, 32),)),
        "w_out": normal_values(keys[4], (HIDDEN_SIZE, OUTW), (2.0 * HIDDEN_SIZE ** -0.5), 0.3046875, ((0, 32),)),
    }


def huber_terms(error_value):
    magnitude = jnp.abs(error_value)
    return jnp.where(magnitude <= 1.0, 0.5 * error_value * error_value, magnitude - 0.5)

def reference(ranges, board, targets, w_in, w_out):
    card_ids = jnp.arange(CARDS, dtype=jnp.int32)
    onehot_board = lax.optimization_barrier(jnp.sum((board[:, :, None] == card_ids[None, None, :]).astype(jnp.float32), axis=1)).astype(jnp.bfloat16)
    features = jnp.concatenate([ranges, onehot_board], axis=1)
    preact = lax.dot_general(features, w_in, (((1,), (1,)), ((), ())), preferred_element_type=jnp.float32)
    hidden = jax.nn.gelu(preact).astype(jnp.bfloat16)
    group_width = HIDDEN_SIZE // N_MP
    summed = jnp.zeros((ranges.shape[0], w_out.shape[1]), jnp.float32)
    for group in range(N_MP):
        part_value = jnp.dot(hidden[:, group * group_width:(group + 1) * group_width], w_out[group * group_width:(group + 1) * group_width], preferred_element_type=jnp.float32)
        rounded = lax.optimization_barrier(part_value.astype(jnp.bfloat16))
        summed = summed + rounded.astype(jnp.float32)
    predicted = summed.astype(jnp.bfloat16)
    error_value = summed - targets.astype(jnp.float32)
    loss = jnp.sum(huber_terms(error_value)) / (ranges.shape[0] * w_out.shape[1])
    out_grad = jnp.clip(error_value, -1.0, 1.0).astype(jnp.bfloat16)
    grad_out = lax.dot_general(hidden, out_grad, (((0,), (0,)), ((), ())), preferred_element_type=jnp.float32)
    hidden_grad = lax.dot_general(out_grad, w_out, (((1,), (1,)), ((), ())), preferred_element_type=jnp.float32)
    unused_value, gelu_back = jax.vjp(jax.nn.gelu, preact)
    preact_grad = gelu_back(hidden_grad)[0].astype(jnp.bfloat16)
    grad_in = lax.dot_general(preact_grad, features, (((0,), (0,)), ((), ())), preferred_element_type=jnp.float32)
    square_sum = jnp.sum(grad_in * grad_in) + jnp.sum(grad_out * grad_out)
    count_params = HIDDEN_SIZE * (w_in.shape[1] + w_out.shape[1])
    scale = lax.rsqrt(square_sum / count_params + 1e-06)
    return (predicted, grad_in * scale, grad_out * scale, loss)
```

```python
import jax
import jax.numpy as jnp
from jax import lax
from jax.sharding import PartitionSpec as P

CARDS = 52


def huber_terms(error_value):
    magnitude = jnp.abs(error_value)
    return jnp.where(magnitude <= 1.0, 0.5 * error_value * error_value, magnitude - 0.5)


def build_features(ranges, board):
    card_ids = jnp.arange(CARDS, dtype=jnp.int32)
    onehot_board = jnp.sum(
        (board[:, :, None] == card_ids[None, None, :]).astype(jnp.float32), axis=1
    ).astype(jnp.bfloat16)
    return jnp.concatenate([ranges, onehot_board], axis=1)


def right_product(left_side, right_block):
    return lax.dot_general(
        left_side, right_block, (((1,), (1,)), ((), ())), preferred_element_type=jnp.float32
    )


def left_product(left_side, right_side):
    return lax.dot_general(
        left_side, right_side, (((0,), (0,)), ((), ())), preferred_element_type=jnp.float32
    )


def gather_weights_body(ranges, board, targets, w_in, w_out):
    mp_count = lax.axis_size("mp")
    dp_count = lax.axis_size("dp")
    stored_rows = ranges.shape[0]
    value_width = w_out.shape[1]
    all_ranges = lax.all_gather(ranges, "mp", axis=0, tiled=True)
    all_board = lax.all_gather(board, "mp", axis=0, tiled=True)
    features = build_features(all_ranges, all_board)
    local_in = lax.all_gather(w_in, "dp", axis=0, tiled=True)
    preact = right_product(features, local_in)
    hidden = jax.nn.gelu(preact).astype(jnp.bfloat16)
    local_out = lax.all_gather(w_out, "dp", axis=0, tiled=True)
    partial_value = jnp.dot(hidden, local_out, preferred_element_type=jnp.float32)
    stacked = partial_value.astype(jnp.bfloat16).reshape(mp_count, stored_rows, value_width)
    received = lax.all_to_all(stacked, "mp", split_axis=0, concat_axis=0, tiled=True)
    summed = jnp.sum(received.astype(jnp.float32), axis=0)
    error_value = summed - targets.astype(jnp.float32)
    own_grad = jnp.clip(error_value, -1.0, 1.0).astype(jnp.bfloat16)
    out_grad = lax.all_gather(own_grad, "mp", axis=0, tiled=True)
    predicted = summed.astype(jnp.bfloat16)
    loss_part = jnp.sum(huber_terms(error_value))
    grad_out = lax.psum_scatter(
        left_product(hidden, out_grad), "dp", scatter_dimension=0, tiled=True
    )
    hidden_grad = right_product(out_grad, local_out)
    unused_value, gelu_back = jax.vjp(jax.nn.gelu, preact)
    preact_grad = gelu_back(hidden_grad)[0].astype(jnp.bfloat16)
    grad_in = lax.psum_scatter(
        left_product(preact_grad, features), "dp", scatter_dimension=0, tiled=True
    )
    square_part = jnp.sum(grad_in * grad_in) + jnp.sum(grad_out * grad_out)
    loss_total, square_total = lax.psum((loss_part, square_part), ("dp", "mp"))
    device_count = mp_count * dp_count
    count_params = w_in.shape[0] * device_count * (w_in.shape[1] + value_width)
    scale = lax.rsqrt(square_total / count_params + 1e-06)
    loss = loss_total / (stored_rows * device_count * value_width)
    return (predicted, grad_in * scale, grad_out * scale, loss)


def gather_states_body(ranges, board, targets, w_in, w_out):
    axes = ("dp", "mp")
    device_count = lax.axis_size("dp") * lax.axis_size("mp")
    stored_rows = ranges.shape[0]
    value_width = w_out.shape[1]
    features = lax.all_gather(build_features(ranges, board), axes, axis=0, tiled=True)
    preact = right_product(features, w_in)
    hidden = jax.nn.gelu(preact).astype(jnp.bfloat16)
    partial_value = jnp.dot(hidden, w_out, preferred_element_type=jnp.float32)
    summed = lax.psum_scatter(
        partial_value.astype(jnp.bfloat16), axes, scatter_dimension=0, tiled=True
    ).astype(jnp.float32)
    error_value = summed - targets.astype(jnp.float32)
    own_grad = jnp.clip(error_value, -1.0, 1.0).astype(jnp.bfloat16)
    out_grad = lax.all_gather(own_grad, axes, axis=0, tiled=True)
    predicted = summed.astype(jnp.bfloat16)
    loss_part = jnp.sum(huber_terms(error_value))
    grad_out = left_product(hidden, out_grad)
    hidden_grad = right_product(out_grad, w_out)
    unused_value, gelu_back = jax.vjp(jax.nn.gelu, preact)
    preact_grad = gelu_back(hidden_grad)[0].astype(jnp.bfloat16)
    grad_in = left_product(preact_grad, features)
    square_part = jnp.sum(grad_in * grad_in) + jnp.sum(grad_out * grad_out)
    loss_total, square_total = lax.psum((loss_part, square_part), axes)
    count_params = w_in.shape[0] * device_count * (w_in.shape[1] + value_width)
    scale = lax.rsqrt(square_total / count_params + 1e-06)
    loss = loss_total / (stored_rows * device_count * value_width)
    return (predicted, grad_in * scale, grad_out * scale, loss)


def solution(mesh):
    rows = P(("dp", "mp"), None)
    units = P(("mp", "dp"), None)

    def step(ranges, board, targets, w_in, w_out):
        batch_fits = ranges.shape[0] <= w_in.shape[0] // mesh.shape["mp"]
        body = gather_states_body if batch_fits else gather_weights_body
        mapped = jax.shard_map(
            body,
            mesh=mesh,
            in_specs=(rows, rows, rows, units, units),
            out_specs=(rows, units, units, P()),
            check_vma=False,
        )
        return mapped(ranges, board, targets, w_in, w_out)

    return step
```

```python
import jax
import jax.numpy as jnp
from jax import lax
from jax.sharding import PartitionSpec as P

CARDS = 52


def huber_terms(error_value):
    magnitude = jnp.abs(error_value)
    return jnp.where(magnitude <= 1.0, 0.5 * error_value * error_value, magnitude - 0.5)


def build_features(ranges, board):
    card_ids = jnp.arange(CARDS, dtype=jnp.int32)
    onehot_board = jnp.sum(
        (board[:, :, None] == card_ids[None, None, :]).astype(jnp.float32), axis=1
    ).astype(jnp.bfloat16)
    return jnp.concatenate([ranges, onehot_board], axis=1)


def right_product(left_side, right_block):
    return lax.dot_general(
        left_side, right_block, (((1,), (1,)), ((), ())), preferred_element_type=jnp.float32
    )


def left_product(left_side, right_side):
    return lax.dot_general(
        left_side, right_side, (((0,), (0,)), ((), ())), preferred_element_type=jnp.float32
    )


def gather_weights_body(ranges, board, targets, w_in, w_out):
    mp_count = lax.axis_size("mp")
    dp_count = lax.axis_size("dp")
    stored_rows = ranges.shape[0]
    value_width = w_out.shape[1]
    all_ranges = lax.all_gather(ranges, "mp", axis=0, tiled=True)
    all_board = lax.all_gather(board, "mp", axis=0, tiled=True)
    features = build_features(all_ranges, all_board)
    local_in = lax.all_gather(w_in, "dp", axis=0, tiled=True)
    preact = right_product(features, local_in)
    hidden = jax.nn.gelu(preact).astype(jnp.bfloat16)
    local_out = lax.all_gather(w_out, "dp", axis=0, tiled=True)
    partial_value = jnp.dot(hidden, local_out, preferred_element_type=jnp.float32)
    stacked = partial_value.astype(jnp.bfloat16).reshape(mp_count, stored_rows, value_width)
    received = lax.all_to_all(stacked, "mp", split_axis=0, concat_axis=0, tiled=True)
    summed = jnp.sum(received.astype(jnp.float32), axis=0)
    error_value = summed - targets.astype(jnp.float32)
    own_grad = jnp.clip(error_value, -1.0, 1.0).astype(jnp.bfloat16)
    out_grad = lax.all_gather(own_grad, "mp", axis=0, tiled=True)
    predicted = summed.astype(jnp.bfloat16)
    loss_part = jnp.sum(huber_terms(error_value))
    grad_out = lax.psum_scatter(
        left_product(hidden, out_grad), "dp", scatter_dimension=0, tiled=True
    )
    hidden_grad = right_product(out_grad, local_out)
    unused_value, gelu_back = jax.vjp(jax.nn.gelu, preact)
    preact_grad = gelu_back(hidden_grad)[0].astype(jnp.bfloat16)
    grad_in = lax.psum_scatter(
        left_product(preact_grad, features), "dp", scatter_dimension=0, tiled=True
    )
    square_part = jnp.sum(grad_in * grad_in) + jnp.sum(grad_out * grad_out)
    loss_total, square_total = lax.psum((loss_part, square_part), ("dp", "mp"))
    device_count = mp_count * dp_count
    count_params = w_in.shape[0] * device_count * (w_in.shape[1] + value_width)
    scale = lax.rsqrt(square_total / count_params + 1e-06)
    loss = loss_total / (stored_rows * device_count * value_width)
    return (predicted, grad_in * scale, grad_out * scale, loss)


def exchange(block, axes, step):
    count = lax.axis_size(axes)
    return lax.ppermute(block, axes, [(index, index ^ step) for index in range(count)])


def gather_blocks(block, axes):
    return [block] + [exchange(block, axes, step) for step in range(1, lax.axis_size(axes))]


def scatter_sum(blocks, axes):
    total = blocks[0]
    received = [
        exchange(blocks[step].astype(jnp.bfloat16), axes, step)
        for step in range(1, lax.axis_size(axes))
    ]
    for part in received:
        total = total + part.astype(jnp.float32)
    return total


def split_rows(whole, count):
    size = whole.shape[0] // count
    return [whole[index * size : (index + 1) * size] for index in range(count)]


def gather_states(rows):
    near = gather_blocks(rows, ("z",))
    far = [exchange(block, ("c",), 1) for block in near]
    return jnp.concatenate(near + far, axis=0)


def torus_body(ranges, board, targets, w_in, w_out):
    plane = ("x", "y")
    z_count = lax.axis_size("z")
    plane_count = lax.axis_size(plane)
    device_count = z_count * plane_count * lax.axis_size("c")
    stored_rows = ranges.shape[0]
    value_width = w_out.shape[1]
    units_in = jnp.concatenate(gather_blocks(w_in, plane), axis=0)
    features = gather_states(build_features(ranges, board))
    units_out = jnp.concatenate(gather_blocks(w_out, plane), axis=0)
    preact = right_product(features, units_in)
    hidden = jax.nn.gelu(preact).astype(jnp.bfloat16)
    partial_value = jnp.dot(hidden, units_out, preferred_element_type=jnp.float32)
    own_half, other_half = split_rows(partial_value, 2)
    chip_value = own_half + exchange(other_half.astype(jnp.bfloat16), ("c",), 1).astype(jnp.float32)
    summed = scatter_sum(split_rows(chip_value, z_count), ("z",))
    error_value = summed - targets.astype(jnp.float32)
    out_grad = gather_states(jnp.clip(error_value, -1.0, 1.0).astype(jnp.bfloat16))
    predicted = summed.astype(jnp.bfloat16)
    loss_part = jnp.sum(huber_terms(error_value))
    grad_out = scatter_sum(split_rows(left_product(hidden, out_grad), plane_count), plane)
    hidden_grad = right_product(out_grad, units_out)
    unused_value, gelu_back = jax.vjp(jax.nn.gelu, preact)
    preact_grad = gelu_back(hidden_grad)[0].astype(jnp.bfloat16)
    grad_in = scatter_sum(split_rows(left_product(preact_grad, features), plane_count), plane)
    square_part = jnp.sum(grad_in * grad_in) + jnp.sum(grad_out * grad_out)
    lane = lax.broadcasted_iota(jnp.int32, (device_count, 128), 1)
    copies = jnp.where(lane == 0, square_part, jnp.where(lane == 1, loss_part, 0.0))
    totals = jnp.sum(
        lax.all_to_all(copies, ("z", "x", "c", "y"), split_axis=0, concat_axis=0, tiled=True), axis=0
    )
    count_params = w_in.shape[0] * device_count * (w_in.shape[1] + value_width)
    scale = lax.rsqrt(totals[0] / count_params + 1e-06)
    loss = totals[1] / (stored_rows * device_count * value_width)
    return (predicted, grad_in * scale, grad_out * scale, loss)


def torus_mesh(mesh):
    devices = mesh.devices
    chips = [tuple(device.coords) for device in devices.flat]
    z_count = len({chip[2] for chip in chips})
    x_count = len({chip[0] for chip in chips})
    core_count = devices.size // len(set(chips))
    shape = (z_count, x_count, core_count, devices.shape[1])
    return jax.sharding.Mesh(devices.reshape(shape), ("z", "x", "c", "y"))


def solution(mesh):
    def step(ranges, board, targets, w_in, w_out):
        batch_fits = ranges.shape[0] <= w_in.shape[0] // mesh.shape["mp"]
        if batch_fits:
            used_mesh, body = torus_mesh(mesh), torus_body
            rows, units = P(("z", "x", "c", "y"), None), P(("y", "z", "x", "c"), None)
        else:
            used_mesh, body = mesh, gather_weights_body
            rows, units = P(("dp", "mp"), None), P(("mp", "dp"), None)
        mapped = jax.shard_map(
            body,
            mesh=used_mesh,
            in_specs=(rows, rows, rows, units, units),
            out_specs=(rows, units, units, P()),
            check_vma=False,
        )
        return mapped(ranges, board, targets, w_in, w_out)

    return step
```

```python
import functools

import jax
import jax.numpy as jnp
from jax import lax
from jax.experimental import pallas as pl
from jax.experimental.pallas import tpu as pltpu
from jax.sharding import PartitionSpec as P

CARDS = 52


def huber_terms(error_value):
    magnitude = jnp.abs(error_value)
    return jnp.where(magnitude <= 1.0, 0.5 * error_value * error_value, magnitude - 0.5)


def build_features(ranges, board):
    card_ids = jnp.arange(CARDS, dtype=jnp.int32)
    onehot_board = jnp.sum(
        (board[:, :, None] == card_ids[None, None, :]).astype(jnp.float32), axis=1
    ).astype(jnp.bfloat16)
    return jnp.concatenate([ranges, onehot_board], axis=1)


def right_product(left_side, right_block):
    return lax.dot_general(
        left_side, right_block, (((1,), (1,)), ((), ())), preferred_element_type=jnp.float32
    )


def left_product(left_side, right_side):
    return lax.dot_general(
        left_side, right_side, (((0,), (0,)), ((), ())), preferred_element_type=jnp.float32
    )


def gather_weights_body(ranges, board, targets, w_in, w_out):
    mp_count = lax.axis_size("mp")
    dp_count = lax.axis_size("dp")
    stored_rows = ranges.shape[0]
    value_width = w_out.shape[1]
    all_ranges = lax.all_gather(ranges, "mp", axis=0, tiled=True)
    all_board = lax.all_gather(board, "mp", axis=0, tiled=True)
    features = build_features(all_ranges, all_board)
    local_in = lax.all_gather(w_in, "dp", axis=0, tiled=True)
    preact = right_product(features, local_in)
    hidden = jax.nn.gelu(preact).astype(jnp.bfloat16)
    local_out = lax.all_gather(w_out, "dp", axis=0, tiled=True)
    partial_value = jnp.dot(hidden, local_out, preferred_element_type=jnp.float32)
    stacked = partial_value.astype(jnp.bfloat16).reshape(mp_count, stored_rows, value_width)
    received = lax.all_to_all(stacked, "mp", split_axis=0, concat_axis=0, tiled=True)
    summed = jnp.sum(received.astype(jnp.float32), axis=0)
    error_value = summed - targets.astype(jnp.float32)
    own_grad = jnp.clip(error_value, -1.0, 1.0).astype(jnp.bfloat16)
    out_grad = lax.all_gather(own_grad, "mp", axis=0, tiled=True)
    predicted = summed.astype(jnp.bfloat16)
    loss_part = jnp.sum(huber_terms(error_value))
    grad_out = lax.psum_scatter(
        left_product(hidden, out_grad), "dp", scatter_dimension=0, tiled=True
    )
    hidden_grad = right_product(out_grad, local_out)
    unused_value, gelu_back = jax.vjp(jax.nn.gelu, preact)
    preact_grad = gelu_back(hidden_grad)[0].astype(jnp.bfloat16)
    grad_in = lax.psum_scatter(
        left_product(preact_grad, features), "dp", scatter_dimension=0, tiled=True
    )
    square_part = jnp.sum(grad_in * grad_in) + jnp.sum(grad_out * grad_out)
    loss_total, square_total = lax.psum((loss_part, square_part), ("dp", "mp"))
    device_count = mp_count * dp_count
    count_params = w_in.shape[0] * device_count * (w_in.shape[1] + value_width)
    scale = lax.rsqrt(square_total / count_params + 1e-06)
    loss = loss_total / (stored_rows * device_count * value_width)
    return (predicted, grad_in * scale, grad_out * scale, loss)


def exchange(block, axes, step):
    count = lax.axis_size(axes)
    return lax.ppermute(block, axes, [(index, index ^ step) for index in range(count)])


def gather_blocks(block, axes):
    return [block] + [exchange(block, axes, step) for step in range(1, lax.axis_size(axes))]


def scatter_sum(blocks, axes):
    total = blocks[0]
    received = [
        exchange(blocks[step].astype(jnp.bfloat16), axes, step)
        for step in range(1, lax.axis_size(axes))
    ]
    for part in received:
        total = total + part.astype(jnp.float32)
    return total


def split_rows(whole, count):
    size = whole.shape[0] // count
    return [whole[index * size : (index + 1) * size] for index in range(count)]


def gather_states(rows):
    near = gather_blocks(rows, ("z",))
    far = [exchange(block, ("c",), 1) for block in near]
    return jnp.concatenate(near + far, axis=0)


def first_hops(weights):
    upper, lower = split_rows(weights, 2)
    return upper, exchange(upper, ("y",), 1), lower, exchange(lower, ("x",), 1)


def second_hops(upper, upper_y, lower, lower_x):
    upper_pair = jnp.concatenate([upper, upper_y], axis=0)
    lower_pair = jnp.concatenate([lower, lower_x], axis=0)
    upper_far = exchange(upper_pair, ("x",), 1)
    lower_far = exchange(lower_pair, ("y",), 1)
    return jnp.concatenate([upper_pair, upper_far, lower_pair, lower_far], axis=0)


def plane_sum(whole):
    upper_pair, upper_far, lower_pair, lower_far = split_rows(whole, 4)
    upper_got = exchange(upper_far.astype(jnp.bfloat16), ("x",), 1)
    lower_got = exchange(lower_far.astype(jnp.bfloat16), ("y",), 1)
    upper_own, upper_next = split_rows(upper_pair, 2)
    lower_own, lower_next = split_rows(lower_pair, 2)
    upper_got_own, upper_got_next = split_rows(upper_got, 2)
    lower_got_own, lower_got_next = split_rows(lower_got, 2)
    upper_next = (upper_next + upper_got_next.astype(jnp.float32)).astype(jnp.bfloat16)
    lower_next = (lower_next + lower_got_next.astype(jnp.float32)).astype(jnp.bfloat16)
    upper_last = exchange(upper_next, ("y",), 1)
    lower_last = exchange(lower_next, ("x",), 1)
    upper_near = upper_own + upper_got_own.astype(jnp.float32)
    lower_near = lower_own + lower_got_own.astype(jnp.float32)
    return jnp.concatenate([upper_near, lower_near], axis=0), upper_last, lower_last


def add_last(near, upper_last, lower_last):
    half = near.shape[0] // 2
    upper = near[:half] + upper_last.astype(jnp.float32)
    lower = near[half:] + lower_last.astype(jnp.float32)
    return upper, lower


def closing_kernel(near, upper_last, lower_last, square_out, loss_part, grad_in, copies):
    upper, lower = add_last(near[...], upper_last[...], lower_last[...])
    half = upper.shape[0]
    grad_in[:half] = upper
    grad_in[half:] = lower
    square = jnp.sum(upper * upper) + jnp.sum(lower * lower) + square_out[0]
    lane = lax.broadcasted_iota(jnp.int32, copies.shape, 1)
    copies[...] = jnp.where(lane == 0, square, jnp.where(lane == 1, loss_part[0], 0.0))


def scaling_kernel(param_count, value_count, copies, grad_in, grad_out, update_in, update_out, loss):
    lane = lax.broadcasted_iota(jnp.int32, copies.shape, 1)
    values = copies[...]
    square = jnp.sum(jnp.where(lane == 0, values, 0.0), keepdims=True)
    scale = lax.rsqrt(square / param_count + 1e-06)
    update_in[...] = grad_in[...] * scale
    update_out[...] = grad_out[...] * scale
    loss[0] = jnp.sum(jnp.where(lane == 1, values, 0.0)) / value_count


def torus_body(ranges, board, targets, w_in, w_out):
    z_count = lax.axis_size("z")
    device_count = z_count * lax.axis_size(("x", "y", "c"))
    stored_rows = ranges.shape[0]
    value_width = w_out.shape[1]
    hops_in = first_hops(w_in)
    hops_out = first_hops(w_out)
    features = gather_states(build_features(ranges, board))
    units_in = second_hops(*hops_in)
    units_out = second_hops(*hops_out)
    preact = right_product(features, units_in)
    hidden = jax.nn.gelu(preact).astype(jnp.bfloat16)
    partial_value = jnp.dot(hidden, units_out, preferred_element_type=jnp.float32)
    own_half, other_half = split_rows(partial_value, 2)
    chip_value = own_half + exchange(other_half.astype(jnp.bfloat16), ("c",), 1).astype(jnp.float32)
    summed = scatter_sum(split_rows(chip_value, z_count), ("z",))
    error_value = summed - targets.astype(jnp.float32)
    out_grad = gather_states(jnp.clip(error_value, -1.0, 1.0).astype(jnp.bfloat16))
    predicted = summed.astype(jnp.bfloat16)
    loss_part = jnp.sum(huber_terms(error_value))
    whole_out = left_product(hidden, out_grad)
    whole_out, out_grad = lax.optimization_barrier((whole_out, out_grad))
    parts_out = plane_sum(whole_out)
    hidden_grad = right_product(out_grad, units_out)
    unused_value, gelu_back = jax.vjp(jax.nn.gelu, preact)
    preact_grad = gelu_back(hidden_grad)[0].astype(jnp.bfloat16)
    parts_in = plane_sum(left_product(preact_grad, features))
    grad_out = jnp.concatenate(add_last(*parts_out), axis=0)
    square_out = jnp.sum(grad_out * grad_out)
    vector = pl.BlockSpec(memory_space=pltpu.VMEM)
    scalar = pl.BlockSpec(memory_space=pltpu.SMEM)
    grad_in, copies = pl.pallas_call(
        closing_kernel,
        out_shape=(
            jax.ShapeDtypeStruct(w_in.shape, jnp.float32),
            jax.ShapeDtypeStruct((device_count, 128), jnp.float32),
        ),
        in_specs=[vector, vector, vector, scalar, scalar],
        out_specs=(vector, vector),
    )(*parts_in, square_out.reshape(1), loss_part.reshape(1))
    copies = lax.all_to_all(copies, ("z", "x", "c", "y"), split_axis=0, concat_axis=0, tiled=True)
    param_count = w_in.shape[0] * device_count * (w_in.shape[1] + value_width)
    value_count = stored_rows * device_count * value_width
    update_in, update_out, loss = pl.pallas_call(
        functools.partial(scaling_kernel, param_count, value_count),
        out_shape=(
            jax.ShapeDtypeStruct(w_in.shape, jnp.float32),
            jax.ShapeDtypeStruct(w_out.shape, jnp.float32),
            jax.ShapeDtypeStruct((1,), jnp.float32),
        ),
        in_specs=[vector, vector, vector],
        out_specs=(vector, vector, scalar),
    )(copies, grad_in, grad_out)
    return (predicted, update_in, update_out, loss.reshape(()))


def torus_mesh(mesh):
    devices = mesh.devices
    chips = [tuple(device.coords) for device in devices.flat]
    z_count = len({chip[2] for chip in chips})
    x_count = len({chip[0] for chip in chips})
    core_count = devices.size // len(set(chips))
    shape = (z_count, x_count, core_count, devices.shape[1])
    return jax.sharding.Mesh(devices.reshape(shape), ("z", "x", "c", "y"))


def solution(mesh):
    def step(ranges, board, targets, w_in, w_out):
        batch_fits = ranges.shape[0] <= w_in.shape[0] // mesh.shape["mp"]
        if batch_fits:
            used_mesh, body = torus_mesh(mesh), torus_body
            rows, units = P(("z", "x", "c", "y"), None), P(("y", "z", "x", "c"), None)
        else:
            used_mesh, body = mesh, gather_weights_body
            rows, units = P(("dp", "mp"), None), P(("mp", "dp"), None)
        mapped = jax.shard_map(
            body,
            mesh=used_mesh,
            in_specs=(rows, rows, rows, units, units),
            out_specs=(rows, units, units, P()),
            check_vma=False,
        )
        return mapped(ranges, board, targets, w_in, w_out)

    return step
```

```python
import functools

import jax
import jax.numpy as jnp
from jax import lax
from jax.experimental import pallas as pl
from jax.experimental.pallas import tpu as pltpu
from jax.sharding import PartitionSpec as P


CARDS = 52


def huber_terms(error_value):
    magnitude = jnp.abs(error_value)
    return jnp.where(magnitude <= 1.0, 0.5 * error_value * error_value, magnitude - 0.5)


def build_features(ranges, board):
    card_ids = jnp.arange(CARDS, dtype=jnp.int32)
    onehot_board = jnp.sum(
        (board[:, :, None] == card_ids[None, None, :]).astype(jnp.float32), axis=1
    ).astype(jnp.bfloat16)
    return jnp.concatenate([ranges, onehot_board], axis=1)


def right_product(left_side, right_block):
    return lax.dot_general(
        left_side, right_block, (((1,), (1,)), ((), ())), preferred_element_type=jnp.float32
    )


def left_product(left_side, right_side):
    return lax.dot_general(
        left_side, right_side, (((0,), (0,)), ((), ())), preferred_element_type=jnp.float32
    )


def gather_weights_body(ranges, board, targets, w_in, w_out):
    mp_count = lax.axis_size("mp")
    dp_count = lax.axis_size("dp")
    stored_rows = ranges.shape[0]
    value_width = w_out.shape[1]
    all_ranges = lax.all_gather(ranges, "mp", axis=0, tiled=True)
    all_board = lax.all_gather(board, "mp", axis=0, tiled=True)
    features = build_features(all_ranges, all_board)
    local_in = lax.all_gather(w_in, "dp", axis=0, tiled=True)
    preact = right_product(features, local_in)
    hidden = jax.nn.gelu(preact).astype(jnp.bfloat16)
    local_out = lax.all_gather(w_out, "dp", axis=0, tiled=True)
    partial_value = jnp.dot(hidden, local_out, preferred_element_type=jnp.float32)
    stacked = partial_value.astype(jnp.bfloat16).reshape(mp_count, stored_rows, value_width)
    received = lax.all_to_all(stacked, "mp", split_axis=0, concat_axis=0, tiled=True)
    summed = jnp.sum(received.astype(jnp.float32), axis=0)
    error_value = summed - targets.astype(jnp.float32)
    own_grad = jnp.clip(error_value, -1.0, 1.0).astype(jnp.bfloat16)
    out_grad = lax.all_gather(own_grad, "mp", axis=0, tiled=True)
    predicted = summed.astype(jnp.bfloat16)
    loss_part = jnp.sum(huber_terms(error_value))
    grad_out = lax.psum_scatter(
        left_product(hidden, out_grad), "dp", scatter_dimension=0, tiled=True
    )
    hidden_grad = right_product(out_grad, local_out)
    _, gelu_back = jax.vjp(jax.nn.gelu, preact)
    preact_grad = gelu_back(hidden_grad)[0].astype(jnp.bfloat16)
    grad_in = lax.psum_scatter(
        left_product(preact_grad, features), "dp", scatter_dimension=0, tiled=True
    )
    square_part = jnp.sum(grad_in * grad_in) + jnp.sum(grad_out * grad_out)
    loss_total, square_total = lax.psum((loss_part, square_part), ("dp", "mp"))
    device_count = mp_count * dp_count
    count_params = w_in.shape[0] * device_count * (w_in.shape[1] + value_width)
    scale = lax.rsqrt(square_total / count_params + 1e-06)
    loss = loss_total / (stored_rows * device_count * value_width)
    return (predicted, grad_in * scale, grad_out * scale, loss)


def exchange(block, axes, step):
    count = lax.axis_size(axes)
    return lax.ppermute(block, axes, [(index, index ^ step) for index in range(count)])


def split_rows(whole, count):
    size = whole.shape[0] // count
    return [whole[index * size : (index + 1) * size] for index in range(count)]


def gather_states(rows):
    near = [rows]
    for step in range(1, lax.axis_size("z")):
        near.append(exchange(rows, ("z",), step))
    far = []
    for block in near:
        far.append(exchange(block, ("c",), 1))
    return jnp.concatenate(near + far, axis=0)


def gather_units(w_in, w_out):
    in_y = exchange(w_in, ("y",), 1)
    out_x = exchange(w_out, ("x",), 1)
    in_x = exchange(w_in, ("x",), 1)
    out_y = exchange(w_out, ("y",), 1)
    in_xy = exchange(in_y, ("x",), 1)
    out_xy = exchange(out_x, ("y",), 1)

    def ordered(own, along_x, along_y, diagonal):
        own, along_x, along_y, diagonal = (split_rows(rows, 2) for rows in (own, along_x, along_y, diagonal))
        first = [own[0], along_y[0], along_x[0], diagonal[0]]
        return jnp.concatenate(first + [own[1], along_x[1], along_y[1], diagonal[1]], axis=0)

    return ordered(w_in, in_x, in_y, in_xy), ordered(w_out, out_x, out_y, out_xy)


def plane_sum(left, right):
    upper_pair, upper_far, lower_pair, lower_far = (block.T for block in split_rows(left.T, 4))
    upper_got = exchange(left_product(upper_far, right).astype(jnp.bfloat16), ("x",), 1)
    lower_got = exchange(left_product(lower_far, right).astype(jnp.bfloat16), ("y",), 1)
    upper_own, upper_next = split_rows(left_product(upper_pair, right), 2)
    lower_own, lower_next = split_rows(left_product(lower_pair, right), 2)
    upper_got_own, upper_got_next = split_rows(upper_got, 2)
    lower_got_own, lower_got_next = split_rows(lower_got, 2)
    upper_next = (upper_next + upper_got_next.astype(jnp.float32)).astype(jnp.bfloat16)
    lower_next = (lower_next + lower_got_next.astype(jnp.float32)).astype(jnp.bfloat16)
    upper_last = exchange(upper_next, ("y",), 1)
    lower_last = exchange(lower_next, ("x",), 1)
    upper_near = upper_own + upper_got_own.astype(jnp.float32)
    lower_near = lower_own + lower_got_own.astype(jnp.float32)
    return upper_near, upper_last, lower_near, lower_last


def closing_kernel(*refs):
    loss_part, grad_in, grad_out, copies = refs[8:]
    square = 0.0
    for parts, grad in ((refs[:4], grad_in), (refs[4:8], grad_out)):
        half = grad.shape[0] // 2
        for index in range(2):
            near, last = parts[2 * index : 2 * index + 2]
            total = near[...] + last[...].astype(jnp.float32)
            grad[index * half : (index + 1) * half] = total
            square = square + jnp.sum(total * total)
    lane = lax.broadcasted_iota(jnp.int32, copies.shape, 1)
    copies[...] = jnp.where(lane == 0, square, jnp.where(lane == 1, loss_part[0], 0.0))


def scaling_kernel(param_count, value_count, copies, grad_in, grad_out, update_in, update_out, loss):
    lane = lax.broadcasted_iota(jnp.int32, copies.shape, 1)
    values = copies[...]
    square = jnp.sum(jnp.where(lane == 0, values, 0.0), keepdims=True)
    scale = lax.rsqrt(square / param_count + 1e-06)
    update_in[...] = grad_in[...] * scale
    update_out[...] = grad_out[...] * scale
    loss[0] = jnp.sum(jnp.where(lane == 1, values, 0.0)) / value_count


def in_vmem(array):
    return pltpu.with_memory_space_constraint(array, pltpu.VMEM)


def torus_body(ranges, board, targets, w_in, w_out):
    z_count = lax.axis_size("z")
    device_count = z_count * lax.axis_size(("x", "y", "c"))
    stored_rows = ranges.shape[0]
    value_width = w_out.shape[1]
    units_in, units_out = gather_units(w_in, w_out)
    features = gather_states(build_features(ranges, board))
    preact = right_product(features, units_in)
    hidden = jax.nn.gelu(preact).astype(jnp.bfloat16)
    own_hidden, other_hidden = split_rows(hidden, 2)
    other_value = jnp.dot(other_hidden, units_out, preferred_element_type=jnp.float32).astype(jnp.bfloat16)
    other_got = exchange(other_value, ("c",), 1)
    own_value = jnp.dot(own_hidden, units_out, preferred_element_type=jnp.float32)
    chip_value = split_rows(own_value + other_got.astype(jnp.float32), z_count)
    summed = chip_value[0]
    received = [exchange(chip_value[k].astype(jnp.bfloat16), ("z",), k) for k in range(1, z_count)]
    for part in received:
        summed = summed + part.astype(jnp.float32)
    error_value = summed - targets.astype(jnp.float32)
    out_grad = gather_states(jnp.clip(error_value, -1.0, 1.0).astype(jnp.bfloat16))
    predicted = summed.astype(jnp.bfloat16)
    loss_part = jnp.sum(huber_terms(error_value))
    parts_out = plane_sum(hidden, out_grad)
    hidden_grad = right_product(out_grad, units_out)
    _, gelu_back = jax.vjp(jax.nn.gelu, preact)
    preact_grad = lax.optimization_barrier(gelu_back(hidden_grad)[0].astype(jnp.bfloat16))
    parts_in = plane_sum(preact_grad, features)
    vector = pl.BlockSpec(memory_space=pltpu.VMEM)
    scalar = pl.BlockSpec(memory_space=pltpu.SMEM)
    grad_in, grad_out, copies = pl.pallas_call(
        closing_kernel,
        out_shape=(
            pltpu.VMEM(w_in.shape, jnp.float32),
            pltpu.VMEM(w_out.shape, jnp.float32),
            pltpu.VMEM((device_count, 128), jnp.float32),
        ),
        in_specs=[vector] * 8 + [scalar],
        out_specs=(vector, vector, vector),
    )(*(in_vmem(part) for part in parts_in + parts_out), loss_part.reshape(1))
    copies = lax.all_to_all(copies, ("z", "x", "c", "y"), split_axis=0, concat_axis=0, tiled=True)
    param_count = w_in.shape[0] * device_count * (w_in.shape[1] + value_width)
    value_count = stored_rows * device_count * value_width
    update_in, update_out, loss = pl.pallas_call(
        functools.partial(scaling_kernel, param_count, value_count),
        out_shape=(
            jax.ShapeDtypeStruct(w_in.shape, jnp.float32),
            jax.ShapeDtypeStruct(w_out.shape, jnp.float32),
            jax.ShapeDtypeStruct((1,), jnp.float32),
        ),
        in_specs=[vector, vector, vector],
        out_specs=(vector, vector, scalar),
    )(in_vmem(copies), in_vmem(grad_in), in_vmem(grad_out))
    return (predicted, update_in, update_out, loss.reshape(()))


def layer_body(*arrays):
    return torus_body(*arrays)


def torus_mesh(mesh):
    devices = mesh.devices
    chips = [tuple(device.coords) for device in devices.flat]
    z_count = len({chip[2] for chip in chips})
    x_count = len({chip[0] for chip in chips})
    core_count = devices.size // len(set(chips))
    shape = (z_count, x_count, core_count, devices.shape[1])
    return jax.sharding.Mesh(devices.reshape(shape), ("z", "x", "c", "y"))


def solution(mesh):
    def step(ranges, board, targets, w_in, w_out):
        batch_fits = ranges.shape[0] <= w_in.shape[0] // mesh.shape["mp"]
        if batch_fits:
            used_mesh, body = torus_mesh(mesh), layer_body
            rows, units = P(("z", "x", "c", "y"), None), P(("y", "z", "x", "c"), None)
        else:
            used_mesh, body = mesh, gather_weights_body
            rows, units = P(("dp", "mp"), None), P(("mp", "dp"), None)
        mapped = jax.shard_map(
            body,
            mesh=used_mesh,
            in_specs=(rows, rows, rows, units, units),
            out_specs=(rows, units, units, P()),
            check_vma=False,
        )
        return mapped(ranges, board, targets, w_in, w_out)

    return step
```

```python
import functools

import jax
import jax.numpy as jnp
from jax import lax
from jax.experimental import pallas as pl
from jax.experimental.pallas import tpu as pltpu
from jax.sharding import PartitionSpec as P


CARDS = 52


def huber_terms(error_value):
    magnitude = jnp.abs(error_value)
    return jnp.where(magnitude <= 1.0, 0.5 * error_value * error_value, magnitude - 0.5)


def build_features(ranges, board):
    card_ids = jnp.arange(CARDS, dtype=jnp.int32)
    onehot_board = jnp.sum(
        (board[:, :, None] == card_ids[None, None, :]).astype(jnp.float32), axis=1
    ).astype(jnp.bfloat16)
    return jnp.concatenate([ranges, onehot_board], axis=1)


def right_product(left_side, right_block):
    return lax.dot_general(
        left_side, right_block, (((1,), (1,)), ((), ())), preferred_element_type=jnp.float32
    )


def left_product(left_side, right_side):
    return lax.dot_general(
        left_side, right_side, (((0,), (0,)), ((), ())), preferred_element_type=jnp.float32
    )


def gather_weights_body(ranges, board, targets, w_in, w_out):
    mp_count = lax.axis_size("mp")
    dp_count = lax.axis_size("dp")
    stored_rows = ranges.shape[0]
    value_width = w_out.shape[1]
    all_ranges = lax.all_gather(ranges, "mp", axis=0, tiled=True)
    all_board = lax.all_gather(board, "mp", axis=0, tiled=True)
    features = build_features(all_ranges, all_board)
    local_in = lax.all_gather(w_in, "dp", axis=0, tiled=True)
    preact = right_product(features, local_in)
    hidden = jax.nn.gelu(preact).astype(jnp.bfloat16)
    local_out = lax.all_gather(w_out, "dp", axis=0, tiled=True)
    partial_value = jnp.dot(hidden, local_out, preferred_element_type=jnp.float32)
    stacked = partial_value.astype(jnp.bfloat16).reshape(mp_count, stored_rows, value_width)
    received = lax.all_to_all(stacked, "mp", split_axis=0, concat_axis=0, tiled=True)
    summed = jnp.sum(received.astype(jnp.float32), axis=0)
    error_value = summed - targets.astype(jnp.float32)
    own_grad = jnp.clip(error_value, -1.0, 1.0).astype(jnp.bfloat16)
    out_grad = lax.all_gather(own_grad, "mp", axis=0, tiled=True)
    predicted = summed.astype(jnp.bfloat16)
    loss_part = jnp.sum(huber_terms(error_value))
    grad_out = lax.psum_scatter(
        left_product(hidden, out_grad), "dp", scatter_dimension=0, tiled=True
    )
    hidden_grad = right_product(out_grad, local_out)
    _, gelu_back = jax.vjp(jax.nn.gelu, preact)
    preact_grad = gelu_back(hidden_grad)[0].astype(jnp.bfloat16)
    grad_in = lax.psum_scatter(
        left_product(preact_grad, features), "dp", scatter_dimension=0, tiled=True
    )
    square_part = jnp.sum(grad_in * grad_in) + jnp.sum(grad_out * grad_out)
    loss_total, square_total = lax.psum((loss_part, square_part), ("dp", "mp"))
    device_count = mp_count * dp_count
    count_params = w_in.shape[0] * device_count * (w_in.shape[1] + value_width)
    scale = lax.rsqrt(square_total / count_params + 1e-06)
    loss = loss_total / (stored_rows * device_count * value_width)
    return (predicted, grad_in * scale, grad_out * scale, loss)


def exchange(block, axes, step):
    count = lax.axis_size(axes)
    return lax.ppermute(block, axes, [(index, index ^ step) for index in range(count)])


def split_rows(whole, count):
    size = whole.shape[0] // count
    return [whole[index * size : (index + 1) * size] for index in range(count)]


def gather_states(rows):
    near = [rows]
    for step in range(1, lax.axis_size("z")):
        near.append(exchange(rows, ("z",), step))
    far = []
    for block in near:
        far.append(exchange(block, ("c",), 1))
    return near + far


def order_units(own, along_x, along_y, diagonal):
    own, along_x, along_y, diagonal = (split_rows(rows, 2) for rows in (own, along_x, along_y, diagonal))
    first = [own[0], along_y[0], along_x[0], diagonal[0]]
    return jnp.concatenate(first + [own[1], along_x[1], along_y[1], diagonal[1]], axis=0)


def gather_inputs(w_in, w_out, features):
    in_y = exchange(w_in, ("y",), 1)
    out_x = exchange(w_out, ("x",), 1)
    in_x = exchange(w_in, ("x",), 1)
    out_y = exchange(w_out, ("y",), 1)
    in_xy = exchange(in_y, ("x",), 1)
    out_xy = exchange(out_x, ("y",), 1)

    states = gather_states(features)
    in_x, out_y, *states = lax.optimization_barrier((in_x, out_y, *states))
    units_in = order_units(w_in, in_x, in_y, in_xy)
    units_out = order_units(w_out, out_x, out_y, out_xy)
    return units_in, units_out, jnp.concatenate(states, axis=0)


def plane_sum(left, right):
    upper_pair, upper_far, lower_pair, lower_far = (block.T for block in split_rows(left.T, 4))
    upper_got = exchange(left_product(upper_far, right).astype(jnp.bfloat16), ("x",), 1)
    lower_got = exchange(left_product(lower_far, right).astype(jnp.bfloat16), ("y",), 1)
    upper_own, upper_next = split_rows(left_product(upper_pair, right), 2)
    lower_own, lower_next = split_rows(left_product(lower_pair, right), 2)
    upper_got_own, upper_got_next = split_rows(upper_got, 2)
    lower_got_own, lower_got_next = split_rows(lower_got, 2)
    upper_next = (upper_next + upper_got_next.astype(jnp.float32)).astype(jnp.bfloat16)
    lower_next = (lower_next + lower_got_next.astype(jnp.float32)).astype(jnp.bfloat16)
    upper_last = exchange(upper_next, ("y",), 1)
    lower_last = exchange(lower_next, ("x",), 1)
    upper_near = upper_own + upper_got_own.astype(jnp.float32)
    lower_near = lower_own + lower_got_own.astype(jnp.float32)
    return upper_near, upper_last, lower_near, lower_last


def closing_kernel(*refs):
    loss_part, grad_in, grad_out, copies = refs[8:]
    square = 0.0
    for parts, grad in ((refs[:4], grad_in), (refs[4:8], grad_out)):
        half = grad.shape[0] // 2
        for index in range(2):
            near, last = parts[2 * index : 2 * index + 2]
            total = near[...] + last[...].astype(jnp.float32)
            grad[index * half : (index + 1) * half] = total
            square = square + jnp.sum(total * total)
    lane = lax.broadcasted_iota(jnp.int32, copies.shape, 1)
    copies[...] = jnp.where(lane == 0, square, jnp.where(lane == 1, loss_part[0], 0.0))


def scaling_kernel(param_count, value_count, copies, grad_in, grad_out, update_in, update_out, loss):
    lane = lax.broadcasted_iota(jnp.int32, copies.shape, 1)
    values = copies[...]
    square = jnp.sum(jnp.where(lane == 0, values, 0.0), keepdims=True)
    scale = lax.rsqrt(square / param_count + 1e-06)
    update_in[...] = grad_in[...] * scale
    update_out[...] = grad_out[...] * scale
    loss[0] = jnp.sum(jnp.where(lane == 1, values, 0.0)) / value_count


def in_vmem(array):
    return pltpu.with_memory_space_constraint(array, pltpu.VMEM)


def torus_body(ranges, board, targets, w_in, w_out):
    z_count = lax.axis_size("z")
    device_count = z_count * lax.axis_size(("x", "y", "c"))
    stored_rows = ranges.shape[0]
    value_width = w_out.shape[1]
    units_in, units_out, features = gather_inputs(w_in, w_out, build_features(ranges, board))
    preact = right_product(features, units_in)
    hidden = jax.nn.gelu(preact).astype(jnp.bfloat16)
    own_hidden, other_hidden = split_rows(hidden, 2)
    other_value = jnp.dot(other_hidden, units_out, preferred_element_type=jnp.float32).astype(jnp.bfloat16)
    other_got = exchange(other_value, ("c",), 1)
    own_value = jnp.dot(own_hidden, units_out, preferred_element_type=jnp.float32)
    chip_value = split_rows(own_value + other_got.astype(jnp.float32), z_count)
    summed = chip_value[0]
    for step in range(1, z_count):
        summed = summed + exchange(chip_value[step].astype(jnp.bfloat16), ("z",), step).astype(jnp.float32)
    error_value = summed - targets.astype(jnp.float32)
    out_grad = jnp.concatenate(gather_states(jnp.clip(error_value, -1.0, 1.0).astype(jnp.bfloat16)), axis=0)
    predicted = summed.astype(jnp.bfloat16)
    loss_part = jnp.sum(huber_terms(error_value))
    parts_out = plane_sum(hidden, out_grad)
    hidden_grad = right_product(out_grad, units_out)
    _, gelu_back = jax.vjp(jax.nn.gelu, preact)
    preact_grad = lax.optimization_barrier(gelu_back(hidden_grad)[0].astype(jnp.bfloat16))
    parts_in = plane_sum(preact_grad, features)
    vector = pl.BlockSpec(memory_space=pltpu.VMEM)
    scalar = pl.BlockSpec(memory_space=pltpu.SMEM)
    grad_in, grad_out, copies = pl.pallas_call(
        closing_kernel,
        out_shape=(
            pltpu.VMEM(w_in.shape, jnp.float32),
            pltpu.VMEM(w_out.shape, jnp.float32),
            pltpu.VMEM((device_count, 128), jnp.float32),
        ),
        in_specs=[vector] * 8 + [scalar],
        out_specs=(vector, vector, vector),
    )(*(in_vmem(part) for part in parts_in + parts_out), loss_part.reshape(1))
    copies = lax.all_to_all(copies, ("z", "x", "c", "y"), split_axis=0, concat_axis=0, tiled=True)
    param_count = w_in.shape[0] * device_count * (w_in.shape[1] + value_width)
    value_count = stored_rows * device_count * value_width
    update_in, update_out, loss = pl.pallas_call(
        functools.partial(scaling_kernel, param_count, value_count),
        out_shape=(
            jax.ShapeDtypeStruct(w_in.shape, jnp.float32),
            jax.ShapeDtypeStruct(w_out.shape, jnp.float32),
            jax.ShapeDtypeStruct((1,), jnp.float32),
        ),
        in_specs=[vector, vector, vector],
        out_specs=(vector, vector, scalar),
    )(in_vmem(copies), in_vmem(grad_in), in_vmem(grad_out))
    return (predicted, update_in, update_out, loss.reshape(()))


def layer_body(*arrays):
    return torus_body(*arrays)


def torus_mesh(mesh):
    devices = mesh.devices
    chips = [tuple(device.coords) for device in devices.flat]
    z_count = len({chip[2] for chip in chips})
    x_count = len({chip[0] for chip in chips})
    core_count = devices.size // len(set(chips))
    shape = (z_count, x_count, core_count, devices.shape[1])
    return jax.sharding.Mesh(devices.reshape(shape), ("z", "x", "c", "y"))


def solution(mesh):
    def step(ranges, board, targets, w_in, w_out):
        batch_fits = ranges.shape[0] <= w_in.shape[0] // mesh.shape["mp"]
        if batch_fits:
            used_mesh, body = torus_mesh(mesh), layer_body
            rows, units = P(("z", "x", "c", "y"), None), P(("y", "z", "x", "c"), None)
        else:
            used_mesh, body = mesh, gather_weights_body
            rows, units = P(("dp", "mp"), None), P(("mp", "dp"), None)
        mapped = jax.shard_map(
            body,
            mesh=used_mesh,
            in_specs=(rows, rows, rows, units, units),
            out_specs=(rows, units, units, P()),
            check_vma=False,
        )
        return mapped(ranges, board, targets, w_in, w_out)

    return step
```
